32 devices in a mesh: shot: 4 (over x, core), tile: 8 (over z, y).
Axes of the slice: x: 2, y: 2, z: 4, core: 2. Of those that a mesh axis runs over, the one named last changes fastest.
Arguments:
- partials: bfloat16 [32, 8, 512, 512], P(('shot', 'tile')), may hold values from -6 to 6
Outputs:
- filtered: float32 [8, 512, 512], P('shot', 'tile')
The draws below stay inside these ranges and needn't reach their ends.
All inputs are finite; a program needn't handle non-finite values.
Results may differ from the reference program's by a relative error of at most 0.0003.
Values may be sent and summed in bfloat16 or wider, within the bound.
A program may use at most 64 MiB of HBM per device.

```python
import jax
import jax.numpy as jnp
from jax import lax

DEPTH = 8
NX = 512
NY = 512
SHOTS = 32


def block_scale(key, shape, shards, low, high):
    level = 1.0
    for dim, blocks in shards:
        draws = jax.random.uniform(jax.random.fold_in(jax.random.fold_in(key, 6), dim), (blocks,), jnp.float32, low / len(shards), high / len(shards))
        level = level * jnp.repeat(jnp.exp(draws), shape[dim] // blocks).reshape((-1,) + (1,) * (len(shape) - 1 - dim))
    return level


def gaussian(own_key, extent, spread, bound, pieces=(), kind=jnp.bfloat16):
    result = jax.random.normal(own_key, extent, jnp.float32) * spread
    if len(pieces) > 0:
        result = block_scale(own_key, extent, pieces, -0.22, 0.18) * result
    return jnp.clip(result, min=-bound, max=bound).astype(kind)


def setup_inputs(seed: int = 0) -> dict:
    splits = jax.random.split(jax.random.key(seed), 2)
    return {
        "partials": gaussian(splits[0], (SHOTS, DEPTH, NX, NY), 1.0, 6.0, ((0, 32),)),
    }


def reference(partials):

    def add_one(total, piece):
        return (total + piece.astype(jnp.float32), None)
    start = jnp.zeros((DEPTH, NX, NY), jnp.float32)
    stack, unused = lax.scan(add_one, start, partials)
    image = stack / jnp.sqrt(jnp.float32(SHOTS))
    padded = jnp.pad(image, 1)
    beside = padded[2:, 1:-1, 1:-1] + padded[:-2, 1:-1, 1:-1]
    beside = beside + padded[1:-1, 2:, 1:-1] + padded[1:-1, :-2, 1:-1]
    beside = beside + padded[1:-1, 1:-1, 2:] + padded[1:-1, 1:-1, :-2]
    return 6.0 * image - beside
```

```python
import functools

import jax
import jax.numpy as jnp
from jax import lax
from jax.experimental import pallas as pl
from jax.experimental.pallas import tpu as pltpu
from jax.sharding import PartitionSpec as P

MESH = pl.DeviceIdType.MESH
F32 = jnp.float32
TOP = 180.0
TINY = 1e-30


def encode(value, scale):
    w = value * scale
    p = w * w
    p = p * p
    p = p * p
    p = p * p
    return jnp.where(w < 0.0, -p, p).astype(jnp.bfloat16)


def decode(code, scale):
    code = code.astype(F32)
    root = lax.rsqrt(lax.rsqrt(lax.rsqrt(lax.rsqrt(jnp.abs(code))))) * scale
    return jnp.where(code < 0.0, -root, root)


def kernel(groups, members, src, out, own, rp, s1a, s1b, r1a, r1b, s2, r2, s3f, s3, r4,
           lim, lim_c, lim_1, lim_2, lim_3, img, low, high, top, bottom, own_sem,
           cs, cr, p1s, p1r, p2s, p2r, p3s, p3r, ms, mr, ns, nr, hs, hr):
    nd, nz, rows, width = src.shape[2], src.shape[3], src.shape[5], src.shape[6]
    cw = width // 4
    rr = s2.shape[3]
    edge = top.shape[1]
    units = [(j, d, h) for d in range(nd) for h in range(0, rows, rr) for j in range(2)]
    steps = len(units)
    g, t = lax.axis_index("shot"), lax.axis_index("tile")
    x, c = g // 2, g % 2
    z, y = t // 2, t % 2

    def dev(gx, tx):
        return {"shot": gx, "tile": tx}

    x_peer = dev((1 - x) * 2 + c, t)
    c_peer = dev(x * 2 + 1 - c, t)
    y_peer = dev(g, z * 2 + 1 - y)

    def z_peer(o):
        return dev(g, lax.rem(z + o, nz) * 2 + y)

    beside = [
        (g > 0, dev(g - 1, t)),
        (g < groups - 1, dev(g + 1, t)),
        (t > 0, dev(g, t - 1)),
        (t < members - 1, dev(g, t + 1)),
    ]

    barrier = pltpu.get_barrier_semaphore()
    peers = [x_peer, c_peer, y_peer] + [z_peer(o) for o in range(1, nz)]
    count = jnp.int32(len(peers))
    for peer in peers:
        pl.semaphore_signal(barrier, inc=1, device_id=peer, device_id_type=MESH)
    for there, peer in beside:
        count = count + jnp.where(there, 1, 0)

        @pl.when(there)
        def _():
            pl.semaphore_signal(barrier, inc=1, device_id=peer, device_id_type=MESH)
    loads = []
    for d in range(nd):
        for core in range(2):
            i = 2 * d + core
            at = 1 - c if core == 0 else c
            loads.append(pltpu.make_async_copy(src.at[:, at, d], own.at[:, at, d], own_sem.at[i]))
    for copy in loads:
        copy.start()

    def remote(a, b, s, r, peer):
        copy = pltpu.make_async_remote_copy(
            src_ref=a, dst_ref=b, send_sem=s, recv_sem=r, device_id=peer, device_id_type=MESH
        )
        copy.start()
        return copy

    def done(ref, sem):
        pltpu.make_async_copy(ref, ref, sem).wait()

    pair, first, second, third = {}, {}, {}, {}

    def span(k):
        j, d, h = units[k]
        return d, pl.ds(h, rr), pl.ds(2 * j * cw, 2 * cw)

    def kind_cols(kind, k):
        j, d, h = units[k]
        return pl.ds((2 * j + kind) * cw, cw)

    def give(k):
        d, r, w = span(k)
        pair[k] = remote(own.at[:, 1 - c, d, :, :, r, w], rp.at[k], cs.at[0], cr.at[k], c_peer)

    def mine(k, kind, a, b):
        d, r, _ = span(k)
        lanes = pl.ds(kind * cw, cw)
        return own[a, c, d, :, b, r, kind_cols(kind, k)].astype(F32) + rp[k, a, :, b, :, lanes].astype(F32)

    for d in range(nd):
        loads[2 * d].wait()
    pl.semaphore_wait(barrier, count)
    lead = min(4, steps)
    for k in range(lead):
        give(k)
    for d in range(nd):
        loads[2 * d + 1].wait()

    most = None
    for a in range(2):
        for b in range(2):
            for d in range(nd):
                def step(i, most, a=a, b=b, d=d):
                    for e in range(2):
                        block = jnp.abs(own[a, b, d, i, e])
                        for r in range(0, rows, rr):
                            most = jnp.maximum(most, block[r:r + rr])
                    return most
                if most is None:
                    most = jnp.zeros((rr, width), own.dtype)
                most = lax.fori_loop(0, nz, step, most)
    most = jnp.max(most.astype(F32), axis=0, keepdims=True)
    most = jnp.max(most, axis=1, keepdims=True)
    lim[0] = jnp.broadcast_to(jnp.maximum(most, TINY), (rr, cw))
    to_core = remote(lim.at[0], lim_c, ms.at[0], mr.at[0], c_peer)
    for k in range(lead, steps):
        give(k)
    to_core.wait_recv()
    lim[1] = lim[0] + lim_c[...]
    remote(lim.at[1], lim_1.at[0], ms.at[1], mr.at[1], x_peer)
    remote(lim.at[1], lim_1.at[1], ms.at[2], mr.at[2], y_peer)

    def limits(stage):
        if stage == 2:
            for kind, peer in enumerate([y_peer, x_peer]):
                done(lim_1.at[kind], mr.at[1 + kind])
                lim[2 + kind] = lim[1] + lim_1[kind]
                remote(lim.at[2 + kind], lim_2.at[kind], ms.at[3 + kind], mr.at[3 + kind], peer)
        if stage == 3:
            for kind in range(2):
                done(lim_2.at[kind], mr.at[3 + kind])
                lim[4 + kind] = lim[2 + kind] + lim_2[kind]
                for o in range(1, nz):
                    remote(lim.at[4 + kind], lim_3.at[kind, z], ns.at[kind], nr.at[kind], z_peer(o))
        if stage == 4:
            for kind in range(2):
                done(lim_3.at[kind, pl.ds(0, nz - 1)], nr.at[kind])

    def up(ref):
        return (TOP / ref)[None]

    def down(ref):
        return (ref * (1.0 / TOP))[None]

    def p1(k):
        pair[k].wait_recv()
        scale = up(lim[1])
        for b in range(2):
            s1a[k, :, b] = encode(mine(k, 0, 1 - x, b), scale)
        ca = remote(s1a.at[k], r1a.at[k], p1s.at[0], p1r.at[0, k], x_peer)
        for a in range(2):
            s1b[k, a] = encode(mine(k, 1, a, 1 - y), scale)
        cb = remote(s1b.at[k], r1b.at[k], p1s.at[1], p1r.at[1, k], y_peer)
        first[k] = (ca, cb)

    def p2(k):
        a, b = first[k]
        a.wait_recv()
        s2[0, k] = encode(mine(k, 0, x, 1 - y) + decode(r1a[k, :, 1 - y], down(lim_1[0])), up(lim[2]))
        ca = remote(s2.at[0, k], r2.at[0, k], p2s.at[0], p2r.at[0, k], y_peer)
        b.wait_recv()
        s2[1, k] = encode(mine(k, 1, 1 - x, y) + decode(r1b[k, 1 - x], down(lim_1[1])), up(lim[3]))
        cb = remote(s2.at[1, k], r2.at[1, k], p2s.at[1], p2r.at[1, k], x_peer)
        second[k] = (ca, cb)

    def p3(k):
        for kind in range(2):
            lanes = pl.ds(kind * cw, cw)
            if kind == 0:
                total = mine(k, 0, x, y) + decode(r1a[k, :, y], down(lim_1[0]))
            else:
                total = mine(k, 1, x, y) + decode(r1b[k, x], down(lim_1[1]))
            second[k][kind].wait_recv()
            total = total + decode(r2[kind, k], down(lim_2[kind]))
            s3f[k, :, :, lanes] = total
            s3[k, :, :, lanes] = encode(total, up(lim[4 + kind]))
        copies = []
        for o in range(1, nz):
            to = lax.rem(z + o, nz)
            copies.append(remote(s3.at[k, to], r4.at[k, z], p3s.at[0], p3r.at[k], z_peer(o)))
        third[k] = copies

    shrink = 1.0 / jnp.sqrt(F32(groups * members))

    def halo(side, a, b):
        there, peer = beside[side]

        @pl.when(there)
        def _():
            remote(a, b, hs.at[side], hr.at[side], peer)

    def last(k):
        j, d, h = units[k]
        _, r, w = span(k)
        done(r4.at[k, pl.ds(0, nz - 1)], p3r.at[k])
        for kind in range(2):
            lanes = pl.ds(kind * cw, cw)
            total = s3f[k, z, :, lanes]
            for o in range(1, nz):
                at = lax.rem(z + nz - o, nz)
                total = total + decode(r4[k, at, :, lanes], lim_3[kind, at] * (1.0 / TOP))
            img[d, r, kind_cols(kind, k)] = total * shrink
        if d == 0:
            halo(0, img.at[d, r, w], high.at[r, w])
        if d == nd - 1:
            halo(1, img.at[d, r, w], low.at[r, w])
        if h == 0:
            halo(2, img.at[d, pl.ds(0, edge), w], bottom.at[d, :, w])
        if h + rr == rows:
            halo(3, img.at[d, pl.ds(rows - edge, edge), w], top.at[d, :, w])

    ahead, lag3, lag4 = 3, 2, 5
    for k in range(min(ahead, steps)):
        p1(k)
    limits(2)
    for k in range(steps + lag4):
        if k < steps:
            p2(k)
        if k + ahead < steps:
            p1(k + ahead)
        if k == min(1, steps - 1):
            limits(3)
        if 0 <= k - lag3 < steps:
            p3(k - lag3)
        if k == lag4:
            limits(4)
        if 0 <= k - lag4 < steps:
            last(k - lag4)
    for side, ref in enumerate([high, low, bottom, top]):
        @pl.when(beside[side ^ 1][0])
        def _():
            done(ref, hr.at[side])

    rown = lax.broadcasted_iota(jnp.int32, (rows, width), 0)
    coln = lax.broadcasted_iota(jnp.int32, (rows, width), 1)
    for d in range(nd):
        here = img[d]
        below = img[d - 1] if d > 0 else jnp.where(g > 0, low[...], 0.0)
        above = img[d + 1] if d < nd - 1 else jnp.where(g < groups - 1, high[...], 0.0)
        before = jnp.where(t > 0, top[d, edge - 1:edge, :], 0.0)
        after = jnp.where(t < members - 1, bottom[d, 0:1, :], 0.0)
        near = above + below
        near = near + jnp.where(rown == rows - 1, after, pltpu.roll(here, rows - 1, 0))
        near = near + jnp.where(rown == 0, before, pltpu.roll(here, 1, 0))
        near = near + jnp.where(coln == width - 1, 0.0, pltpu.roll(here, width - 1, 1))
        near = near + jnp.where(coln == 0, 0.0, pltpu.roll(here, 1, 1))
        out[d] = 6.0 * here - near
    for side, ref in enumerate([high, low, bottom, top]):
        @pl.when(beside[side][0])
        def _():
            done(ref, hs.at[side])
    done(rp, cs.at[0])
    done(r1a, p1s.at[0])
    done(r1b, p1s.at[1])
    for kind in range(2):
        done(r2.at[kind], p2s.at[kind])
        done(lim_3.at[kind, pl.ds(0, nz - 1)], ns.at[kind])
    done(r4.at[:, pl.ds(0, nz - 1)], p3s.at[0])
    for i in range(5):
        done(lim_c, ms.at[i])


def body(groups, members, partials):
    shots, depth, lateral, width = partials.shape
    nd, nz, rows, cw = depth // groups, members // 2, lateral // members, width // 4
    parts = 4 if rows % 64 == 0 else 1
    rr, edge = rows // parts, min(8, rows)
    steps = 2 * nd * parts
    src = partials.reshape(2, 2, nd, nz, 2, rows, width)
    kind = partials.dtype
    dma = pltpu.SemaphoreType.DMA
    return pl.pallas_call(
        functools.partial(kernel, groups, members),
        out_shape=jax.ShapeDtypeStruct((nd, rows, width), F32),
        in_specs=[pl.BlockSpec(memory_space=pl.ANY)],
        out_specs=pl.BlockSpec(memory_space=pltpu.VMEM),
        scratch_shapes=[
            pltpu.VMEM((2, 2, nd, nz, 2, rows, width), kind),
            pltpu.VMEM((steps, 2, nz, 2, rr, 2 * cw), kind),
            pltpu.VMEM((steps, nz, 2, rr, cw), kind),
            pltpu.VMEM((steps, 2, nz, rr, cw), kind),
            pltpu.VMEM((steps, nz, 2, rr, cw), kind),
            pltpu.VMEM((steps, 2, nz, rr, cw), kind),
            pltpu.VMEM((2, steps, nz, rr, cw), kind),
            pltpu.VMEM((2, steps, nz, rr, cw), kind),
            pltpu.VMEM((steps, nz, rr, 2 * cw), F32),
            pltpu.VMEM((steps, nz, rr, 2 * cw), kind),
            pltpu.VMEM((steps, nz, rr, 2 * cw), kind),
            pltpu.VMEM((6, rr, cw), F32),
            pltpu.VMEM((rr, cw), F32),
            pltpu.VMEM((2, rr, cw), F32),
            pltpu.VMEM((2, rr, cw), F32),
            pltpu.VMEM((2, nz, rr, cw), F32),
            pltpu.VMEM((nd, rows, width), F32),
            pltpu.VMEM((rows, width), F32),
            pltpu.VMEM((rows, width), F32),
            pltpu.VMEM((nd, edge, width), F32),
            pltpu.VMEM((nd, edge, width), F32),
            dma((2 * nd,)),
            dma((1,)), dma((steps,)),
            dma((2,)), dma((2, steps)),
            dma((2,)), dma((2, steps)),
            dma((1,)), dma((steps,)),
            dma((5,)), dma((5,)),
            dma((2,)), dma((2,)),
            dma((4,)), dma((4,)),
        ],
        compiler_params=pltpu.CompilerParams(collective_id=0, has_side_effects=True),
    )(src)


def solution(mesh):
    groups, members = mesh.shape["shot"], mesh.shape["tile"]
    return jax.shard_map(
        functools.partial(body, groups, members),
        mesh=mesh,
        in_specs=(P(("shot", "tile"), None, None, None),),
        out_specs=P("shot", "tile", None),
        check_vma=False,
    )
```

```python
import functools

import jax
import jax.numpy as jnp
from jax import lax
from jax.experimental import pallas as pl
from jax.experimental.pallas import tpu as pltpu
from jax.sharding import PartitionSpec as P

MESH = pl.DeviceIdType.MESH
F32 = jnp.float32
TOP = 180.0
TINY = 1e-30


def encode(value, scale):
    w = value * scale
    p = w * w
    p = p * p
    p = p * p
    p = p * p
    return jnp.where(w < 0.0, -p, p).astype(jnp.bfloat16)


def decode(code, scale):
    code = code.astype(F32)
    root = lax.rsqrt(lax.rsqrt(lax.rsqrt(lax.rsqrt(jnp.abs(code))))) * scale
    return jnp.where(code < 0.0, -root, root)


def kernel(groups, members, src, out, own, rp, s1a, s1b, r1a, r1b, s2, r2, s3f, s3, r4,
           sz, rz, tz, sw, rw, lim, lim_c, lim_1, lim_2, lim_3, lim_z, lim_w,
           img, low, high, top, bottom, own_sem, cs, cr, p1s, p1r, p2s, p2r, p3s, p3r,
           zs, zr, ws, wr, ms, mr, ns, nr, vs, vr, hs, hr, chain):
    nd, nz, rows, width = src.shape[2], src.shape[3], src.shape[5], src.shape[6]
    cw = width // 4
    rr = s2.shape[3]
    edge = top.shape[1]
    units = [(j, d, h) for d in range(nd) for h in range(0, rows, rr) for j in range(2)]
    early = sz.shape[0]
    at = len(units) * 5 // 8
    late = units[at:at + early]
    units = units[:at] + units[at + early:] + late
    total_steps = len(units)
    steps = total_steps - early
    g, t = lax.axis_index("shot"), lax.axis_index("tile")
    x, c = g // 2, g % 2
    z, y = t // 2, t % 2

    def dev(gx, tx):
        return {"shot": gx, "tile": tx}

    x_peer = dev((1 - x) * 2 + c, t)
    c_peer = dev(x * 2 + 1 - c, t)
    y_peer = dev(g, z * 2 + 1 - y)
    d_peer = dev((1 - x) * 2 + c, z * 2 + 1 - y)

    def z_peer(o):
        return dev(g, lax.rem(z + o, nz) * 2 + y)

    beside = [
        (g > 0, dev(g - 1, t)),
        (g < groups - 1, dev(g + 1, t)),
        (t > 0, dev(g, t - 1)),
        (t < members - 1, dev(g, t + 1)),
    ]

    barrier = pltpu.get_barrier_semaphore()
    near = [(z > 0, dev(g, t - 2)), (z < nz - 1, dev(g, t + 2))]
    peers = [c_peer, x_peer, y_peer]
    count = jnp.int32(len(peers))
    for peer in peers:
        pl.semaphore_signal(barrier, inc=1, device_id=peer, device_id_type=MESH)
    for there, peer in near:
        count = count + jnp.where(there, 1, 0)

        @pl.when(there)
        def _():
            pl.semaphore_signal(barrier, inc=1, device_id=peer, device_id_type=MESH)
    loads = []
    for d in range(nd):
        for core in range(2):
            i = 2 * d + core
            at = 1 - c if core == 0 else c
            loads.append(pltpu.make_async_copy(src.at[:, at, d], own.at[:, at, d], own_sem.at[i]))
    for copy in loads:
        copy.start()

    def remote(a, b, s, r, peer):
        copy = pltpu.make_async_remote_copy(
            src_ref=a, dst_ref=b, send_sem=s, recv_sem=r, device_id=peer, device_id_type=MESH
        )
        copy.start()
        return copy

    def done(ref, sem):
        pltpu.make_async_copy(ref, ref, sem).wait()

    pair, first, second, third = {}, {}, {}, {}

    def span(k):
        j, d, h = units[k]
        return d, pl.ds(h, rr), pl.ds(2 * j * cw, 2 * cw)

    def kind_cols(kind, k):
        j, d, h = units[k]
        return pl.ds((2 * j + kind) * cw, cw)

    def give(k):
        d, r, w = span(k)
        pair[k] = remote(own.at[:, 1 - c, d, :, :, r, w], rp.at[k], cs.at[0], cr.at[k], c_peer)

    def mine(k, kind, a, b):
        d, r, _ = span(k)
        lanes = pl.ds(kind * cw, cw)
        return own[a, c, d, :, b, r, kind_cols(kind, k)].astype(F32) + rp[k, a, :, b, :, lanes].astype(F32)

    for d in range(nd):
        loads[2 * d].wait()
    pl.semaphore_wait(barrier, count)
    order = []
    for k in range(steps):
        order.append(k)
        if k < early:
            order.append(steps + k)
    lead = min(4, len(order))
    for k in order[:lead]:
        give(k)
    for way, (there, peer) in enumerate([near[1], near[0]]):
        behind = z if way == 0 else nz - 1 - z

        @pl.when(behind > 1)
        def _():
            pl.semaphore_wait(chain.at[way], 1)

        @pl.when(jnp.logical_and(there, behind > 0))
        def _():
            pl.semaphore_signal(chain.at[way], inc=1, device_id=peer, device_id_type=MESH)
    for d in range(nd):
        loads[2 * d + 1].wait()

    most = None
    for a in range(2):
        for b in range(2):
            for d in range(nd):
                def step(i, most, a=a, b=b, d=d):
                    for e in range(2):
                        block = jnp.abs(own[a, b, d, i, e])
                        for r in range(0, rows, rr):
                            most = jnp.maximum(most, block[r:r + rr])
                    return most
                if most is None:
                    most = jnp.zeros((rr, width), own.dtype)
                most = lax.fori_loop(0, nz, step, most)
    most = jnp.max(most.astype(F32), axis=0, keepdims=True)
    most = jnp.max(most, axis=1, keepdims=True)
    lim[0] = jnp.broadcast_to(jnp.maximum(most, TINY), (rr, cw))
    to_core = remote(lim.at[0], lim_c, ms.at[0], mr.at[0], c_peer)
    for k in order[lead:]:
        give(k)
    to_core.wait_recv()
    lim[1] = lim[0] + lim_c[...]
    remote(lim.at[1], lim_1.at[0], ms.at[1], mr.at[1], x_peer)
    remote(lim.at[1], lim_1.at[1], ms.at[2], mr.at[2], y_peer)

    def limits(stage):
        if stage == 1 and early:
            for o in range(1, nz):
                remote(lim.at[1], lim_z.at[z], vs.at[0], vr.at[0], z_peer(o))
        if stage == 5 and early:
            done(lim_z.at[pl.ds(0, nz - 1)], vr.at[0])
            most = lim[1]
            for o in range(1, nz):
                most = most + lim_z[lax.rem(z + o, nz)]
            lim[6] = most
            for i, peer in enumerate([d_peer, x_peer, y_peer]):
                remote(lim.at[6], lim_w.at[i], vs.at[1], vr.at[1], peer)
        if stage == 6 and early:
            done(lim_w, vr.at[1])
        if stage == 2:
            for kind, peer in enumerate([y_peer, x_peer]):
                done(lim_1.at[kind], mr.at[1 + kind])
                lim[2 + kind] = lim[1] + lim_1[kind]
                remote(lim.at[2 + kind], lim_2.at[kind], ms.at[3 + kind], mr.at[3 + kind], peer)
        if stage == 3:
            for kind in range(2):
                done(lim_2.at[kind], mr.at[3 + kind])
                lim[4 + kind] = lim[2 + kind] + lim_2[kind]
                for o in range(1, nz):
                    remote(lim.at[4 + kind], lim_3.at[kind, z], ns.at[kind], nr.at[kind], z_peer(o))
        if stage == 4:
            for kind in range(2):
                done(lim_3.at[kind, pl.ds(0, nz - 1)], nr.at[kind])

    def up(ref):
        return (TOP / ref)[None]

    def down(ref):
        return (ref * (1.0 / TOP))[None]

    def p1(k):
        pair[k].wait_recv()
        scale = up(lim[1])
        for b in range(2):
            s1a[k, :, b] = encode(mine(k, 0, 1 - x, b), scale)
        ca = remote(s1a.at[k], r1a.at[k], p1s.at[0], p1r.at[0, k], x_peer)
        for a in range(2):
            s1b[k, a] = encode(mine(k, 1, a, 1 - y), scale)
        cb = remote(s1b.at[k], r1b.at[k], p1s.at[1], p1r.at[1, k], y_peer)
        first[k] = (ca, cb)

    def p2(k):
        a, b = first[k]
        a.wait_recv()
        s2[0, k] = encode(mine(k, 0, x, 1 - y) + decode(r1a[k, :, 1 - y], down(lim_1[0])), up(lim[2]))
        ca = remote(s2.at[0, k], r2.at[0, k], p2s.at[0], p2r.at[0, k], y_peer)
        b.wait_recv()
        s2[1, k] = encode(mine(k, 1, 1 - x, y) + decode(r1b[k, 1 - x], down(lim_1[1])), up(lim[3]))
        cb = remote(s2.at[1, k], r2.at[1, k], p2s.at[1], p2r.at[1, k], x_peer)
        second[k] = (ca, cb)

    def p3(k):
        for kind in range(2):
            lanes = pl.ds(kind * cw, cw)
            if kind == 0:
                total = mine(k, 0, x, y) + decode(r1a[k, :, y], down(lim_1[0]))
            else:
                total = mine(k, 1, x, y) + decode(r1b[k, x], down(lim_1[1]))
            second[k][kind].wait_recv()
            total = total + decode(r2[kind, k], down(lim_2[kind]))
            s3f[k, :, :, lanes] = total
            s3[k, :, :, lanes] = encode(total, up(lim[4 + kind]))
        copies = []
        for o in range(1, nz):
            to = lax.rem(z + o, nz)
            copies.append(remote(s3.at[k, to], r4.at[k, z], p3s.at[0], p3r.at[k], z_peer(o)))
        third[k] = copies

    def z1(i):
        k = steps + i
        pair[k].wait_recv()
        scale = jnp.concatenate([up(lim[1])] * 2, axis=-1)
        d, r, w = span(k)
        for o in range(1, nz):
            to = lax.rem(z + o, nz)
            for a in range(2):
                sz[i, to, a] = encode(own[a, c, d, to, :, r, w].astype(F32) + rp[k, a, to].astype(F32), scale)
            remote(sz.at[i, to], rz.at[i, z], zs.at[0], zr.at[i], z_peer(o))

    def z2(i):
        k = steps + i
        done(rz.at[i, pl.ds(0, nz - 1)], zr.at[i])
        d, r, w = span(k)
        scale = jnp.concatenate([up(lim[6])] * 2, axis=-1)
        for a in range(2):
            total = own[a, c, d, z, :, r, w].astype(F32) + rp[k, a, z].astype(F32)
            for o in range(1, nz):
                of = lax.rem(z + o, nz)
                total = total + decode(rz[i, of, a], jnp.concatenate([down(lim_z[of])] * 2, axis=-1))
            tz[i, a] = total
            sw[i, a] = encode(total, scale)
        for n, (a, b, peer) in enumerate([(1 - x, 1 - y, d_peer), (1 - x, y, x_peer), (x, 1 - y, y_peer)]):
            remote(sw.at[i, a, b], rw.at[i, n], ws.at[0], wr.at[i], peer)

    def z3(i):
        done(rw.at[i], wr.at[i])
        total = tz[i, x, y]
        for n in range(3):
            total = total + decode(rw[i, n], jnp.concatenate([lim_w[n] * (1.0 / TOP)] * 2, axis=-1))
        _, r, w = span(steps + i)
        img[units[steps + i][1], r, w] = total * shrink
        edges(steps + i)

    shrink = 1.0 / jnp.sqrt(F32(groups * members))

    def halo(side, a, b):
        there, peer = beside[side]

        @pl.when(there)
        def _():
            remote(a, b, hs.at[side], hr.at[side], peer)

    def last(k):
        j, d, h = units[k]
        _, r, w = span(k)
        done(r4.at[k, pl.ds(0, nz - 1)], p3r.at[k])
        for kind in range(2):
            lanes = pl.ds(kind * cw, cw)
            total = s3f[k, z, :, lanes]
            for o in range(1, nz):
                at = lax.rem(z + nz - o, nz)
                total = total + decode(r4[k, at, :, lanes], lim_3[kind, at] * (1.0 / TOP))
            img[d, r, kind_cols(kind, k)] = total * shrink
        edges(k)

    def edges(k):
        j, d, h = units[k]
        _, r, w = span(k)
        if d == 0:
            halo(0, img.at[d, r, w], high.at[r, w])
        if d == nd - 1:
            halo(1, img.at[d, r, w], low.at[r, w])
        if h == 0:
            halo(2, img.at[d, pl.ds(0, edge), w], bottom.at[d, :, w])
        if h + rr == rows:
            halo(3, img.at[d, pl.ds(rows - edge, edge), w], top.at[d, :, w])

    ahead, lag3, lag4, at_z2 = 5, 6, 11, 9
    ahead = min(ahead, steps)
    p1(0)
    limits(1)
    for k in range(1, ahead):
        if k <= early:
            z1(k - 1)
        p1(k)
    for i in range(max(ahead - 1, 0), early):
        z1(i)
    limits(2)
    for k in range(steps + lag4):
        if k < steps:
            p2(k)
        if k + ahead < steps:
            p1(k + ahead)
        if k == min(1, steps - 1):
            limits(3)
        if k == min(at_z2, steps - 1):
            limits(5)
            for i in range(early):
                z2(i)
        if 0 <= k - lag3 < steps:
            p3(k - lag3)
        if k == lag4:
            limits(4)
        if k == steps + lag4 - 2:
            limits(6)
            for i in range(early):
                z3(i)
        if 0 <= k - lag4 < steps:
            last(k - lag4)
    for side, ref in enumerate([high, low, bottom, top]):
        @pl.when(beside[side ^ 1][0])
        def _():
            done(ref, hr.at[side])

    rown = lax.broadcasted_iota(jnp.int32, (rows, width), 0)
    coln = lax.broadcasted_iota(jnp.int32, (rows, width), 1)
    for d in range(nd):
        here = img[d]
        below = img[d - 1] if d > 0 else jnp.where(g > 0, low[...], 0.0)
        above = img[d + 1] if d < nd - 1 else jnp.where(g < groups - 1, high[...], 0.0)
        before = jnp.where(t > 0, top[d, edge - 1:edge, :], 0.0)
        after = jnp.where(t < members - 1, bottom[d, 0:1, :], 0.0)
        near = above + below
        near = near + jnp.where(rown == rows - 1, after, pltpu.roll(here, rows - 1, 0))
        near = near + jnp.where(rown == 0, before, pltpu.roll(here, 1, 0))
        near = near + jnp.where(coln == width - 1, 0.0, pltpu.roll(here, width - 1, 1))
        near = near + jnp.where(coln == 0, 0.0, pltpu.roll(here, 1, 1))
        out[d] = 6.0 * here - near
    for side, ref in enumerate([high, low, bottom, top]):
        @pl.when(beside[side][0])
        def _():
            done(ref, hs.at[side])
    done(rp, cs.at[0])
    done(r1a, p1s.at[0])
    done(r1b, p1s.at[1])
    for kind in range(2):
        done(r2.at[kind], p2s.at[kind])
        done(lim_3.at[kind, pl.ds(0, nz - 1)], ns.at[kind])
    done(r4.at[:, pl.ds(0, nz - 1)], p3s.at[0])
    if early:
        done(rz.at[:, pl.ds(0, nz - 1)], zs.at[0])
        done(rw, ws.at[0])
        done(lim_z.at[pl.ds(0, nz - 1)], vs.at[0])
        done(lim_w, vs.at[1])
    for i in range(5):
        done(lim_c, ms.at[i])


def body(groups, members, partials):
    shots, depth, lateral, width = partials.shape
    nd, nz, rows, cw = depth // groups, members // 2, lateral // members, width // 4
    parts = 4 if rows % 64 == 0 else 1
    rr, edge = rows // parts, min(8, rows)
    early = 3 if parts > 1 else 1
    total = 2 * nd * parts
    steps = total - early
    src = partials.reshape(2, 2, nd, nz, 2, rows, width)
    kind = partials.dtype
    dma = pltpu.SemaphoreType.DMA
    return pl.pallas_call(
        functools.partial(kernel, groups, members),
        out_shape=jax.ShapeDtypeStruct((nd, rows, width), F32),
        in_specs=[pl.BlockSpec(memory_space=pl.ANY)],
        out_specs=pl.BlockSpec(memory_space=pltpu.VMEM),
        scratch_shapes=[
            pltpu.VMEM((2, 2, nd, nz, 2, rows, width), kind),
            pltpu.VMEM((total, 2, nz, 2, rr, 2 * cw), kind),
            pltpu.VMEM((steps, nz, 2, rr, cw), kind),
            pltpu.VMEM((steps, 2, nz, rr, cw), kind),
            pltpu.VMEM((steps, nz, 2, rr, cw), kind),
            pltpu.VMEM((steps, 2, nz, rr, cw), kind),
            pltpu.VMEM((2, steps, nz, rr, cw), kind),
            pltpu.VMEM((2, steps, nz, rr, cw), kind),
            pltpu.VMEM((steps, nz, rr, 2 * cw), F32),
            pltpu.VMEM((steps, nz, rr, 2 * cw), kind),
            pltpu.VMEM((steps, nz, rr, 2 * cw), kind),
            pltpu.VMEM((early, nz, 2, 2, rr, 2 * cw), kind),
            pltpu.VMEM((early, nz, 2, 2, rr, 2 * cw), kind),
            pltpu.VMEM((early, 2, 2, rr, 2 * cw), F32),
            pltpu.VMEM((early, 2, 2, rr, 2 * cw), kind),
            pltpu.VMEM((early, 3, rr, 2 * cw), kind),
            pltpu.VMEM((7, rr, cw), F32),
            pltpu.VMEM((rr, cw), F32),
            pltpu.VMEM((2, rr, cw), F32),
            pltpu.VMEM((2, rr, cw), F32),
            pltpu.VMEM((2, nz, rr, cw), F32),
            pltpu.VMEM((nz, rr, cw), F32),
            pltpu.VMEM((3, rr, cw), F32),
            pltpu.VMEM((nd, rows, width), F32),
            pltpu.VMEM((rows, width), F32),
            pltpu.VMEM((rows, width), F32),
            pltpu.VMEM((nd, edge, width), F32),
            pltpu.VMEM((nd, edge, width), F32),
            dma((2 * nd,)),
            dma((1,)), dma((total,)),
            dma((2,)), dma((2, steps)),
            dma((2,)), dma((2, steps)),
            dma((1,)), dma((steps,)),
            dma((1,)), dma((early,)),
            dma((1,)), dma((early,)),
            dma((5,)), dma((5,)),
            dma((2,)), dma((2,)),
            dma((2,)), dma((2,)),
            dma((4,)), dma((4,)),
            pltpu.SemaphoreType.REGULAR((2,)),
        ],
        compiler_params=pltpu.CompilerParams(collective_id=0, has_side_effects=True, vmem_limit_bytes=51 * 2**20),
    )(src)


def solution(mesh):
    groups, members = mesh.shape["shot"], mesh.shape["tile"]
    return jax.shard_map(
        functools.partial(body, groups, members),
        mesh=mesh,
        in_specs=(P(("shot", "tile"), None, None, None),),
        out_specs=P("shot", "tile", None),
        check_vma=False,
    )
```

```python
import functools

import jax
import jax.numpy as jnp
from jax import lax
from jax.experimental import pallas as pl
from jax.experimental.pallas import tpu as pltpu
from jax.sharding import PartitionSpec as P

MESH = pl.DeviceIdType.MESH
F32 = jnp.float32
TOP = 180.0
TINY = 1e-30


def plan(steps, early):
    ahead, lag3, lag4, at_b, at_c = 5, 7, 12, 9, 2
    ahead = min(ahead, steps)
    seq = []
    for k in range(ahead):
        seq.append(("1", k))
        if 1 <= k <= early:
            seq.append(("A", k - 1))
    seq += [("A", k) for k in range(max(ahead - 1, 0), early)]
    for k in range(steps + lag4):
        if k < steps:
            seq.append(("2", k))
        if k + ahead < steps:
            seq.append(("1", k + ahead))
        if k == min(at_b, steps - 1):
            seq += [("B", i) for i in range(early)]
        if 0 <= k - lag3 < steps:
            seq.append(("3", k - lag3))
        if k == steps + lag4 - at_c:
            seq += [("C", i) for i in range(early)]
        if 0 <= k - lag4 < steps:
            seq.append(("4", k - lag4))
    return seq


def encode(value, scale):
    w = value * scale
    p = w * w
    p = p * p
    p = p * p
    p = p * p
    return jnp.where(w < 0.0, -p, p).astype(jnp.bfloat16)


def decode(code, scale):
    code = code.astype(F32)
    root = lax.rsqrt(lax.rsqrt(lax.rsqrt(lax.rsqrt(jnp.abs(code))))) * scale
    return jnp.where(code < 0.0, -root, root)


def kernel(groups, members, src, out, own, rp, s1a, s1b, r1a, r1b, s2, r2, s3f, s3, r4,
           sz, rz, tz, sw, rw, lim, lim_c, lim_1, lim_2, lim_3, lim_z, lim_w,
           img, low, high, top, bottom, own_sem, cs, cr, p1s, p1r, p2s, p2r, p3s, p3r,
           zs, zr, ws, wr, ms, mr, ns, nr, vs, vr, hs, hr, chain):
    nd, nz, rows, width = src.shape[2], src.shape[3], src.shape[5], src.shape[6]
    cw = width // 4
    rr = s2.shape[3]
    edge = top.shape[1]
    units = [(j, d, h) for d in range(nd) for h in range(0, rows, rr) for j in range(2)]
    early = sz.shape[0]
    at = len(units) * 5 // 8
    late = units[at:at + early]
    units = units[:at] + units[at + early:] + late
    total_steps = len(units)
    steps = total_steps - early
    g, t = lax.axis_index("shot"), lax.axis_index("tile")
    x, c = g // 2, g % 2
    z, y = t // 2, t % 2

    def dev(gx, tx):
        return {"shot": gx, "tile": tx}

    x_peer = dev((1 - x) * 2 + c, t)
    c_peer = dev(x * 2 + 1 - c, t)
    y_peer = dev(g, z * 2 + 1 - y)
    d_peer = dev((1 - x) * 2 + c, z * 2 + 1 - y)

    def z_peer(o):
        return dev(g, lax.rem(z + o, nz) * 2 + y)

    beside = [
        (g > 0, dev(g - 1, t)),
        (g < groups - 1, dev(g + 1, t)),
        (t > 0, dev(g, t - 1)),
        (t < members - 1, dev(g, t + 1)),
    ]

    barrier = pltpu.get_barrier_semaphore()
    near = [(z > 0, dev(g, t - 2)), (z < nz - 1, dev(g, t + 2))]
    peers = [c_peer, x_peer, y_peer]
    count = jnp.int32(len(peers))
    for peer in peers:
        pl.semaphore_signal(barrier, inc=1, device_id=peer, device_id_type=MESH)
    for there, peer in near:
        count = count + jnp.where(there, 1, 0)

        @pl.when(there)
        def _():
            pl.semaphore_signal(barrier, inc=1, device_id=peer, device_id_type=MESH)
    loads = []
    for d in range(nd):
        for core in range(2):
            i = 2 * d + core
            at = 1 - c if core == 0 else c
            loads.append(pltpu.make_async_copy(src.at[:, at, d], own.at[:, at, d], own_sem.at[i]))
    for copy in loads:
        copy.start()

    def remote(a, b, s, r, peer):
        copy = pltpu.make_async_remote_copy(
            src_ref=a, dst_ref=b, send_sem=s, recv_sem=r, device_id=peer, device_id_type=MESH
        )
        copy.start()
        return copy

    def done(ref, sem):
        pltpu.make_async_copy(ref, ref, sem).wait()

    pair, first, second, third = {}, {}, {}, {}

    def span(k):
        j, d, h = units[k]
        return d, pl.ds(h, rr), pl.ds(2 * j * cw, 2 * cw)

    def kind_cols(kind, k):
        j, d, h = units[k]
        return pl.ds((2 * j + kind) * cw, cw)

    def give(k):
        d, r, w = span(k)
        pair[k] = remote(own.at[:, 1 - c, d, :, :, r, w], rp.at[k], cs.at[0], cr.at[k], c_peer)

    def mine(k, kind, a, b):
        d, r, _ = span(k)
        lanes = pl.ds(kind * cw, cw)
        return own[a, c, d, :, b, r, kind_cols(kind, k)].astype(F32) + rp[k, a, :, b, :, lanes].astype(F32)

    order = []
    for k in range(steps):
        order.append(k)
        if 1 <= k <= early:
            order.append(steps + k - 1)
    lead = 2
    most = jnp.zeros((rr, width), own.dtype)
    for d in range(nd):
        for core in range(2):
            loads[2 * d + core].wait()
            if d == 0 and core == 0:
                pl.semaphore_wait(barrier, count)
                for k in order[:lead]:
                    give(k)
            at = 1 - c if core == 0 else c
            for a in range(2):
                def step(i, most, a=a, at=at, d=d):
                    for b in range(2):
                        block = jnp.abs(own[a, at, d, i, b])
                        for r in range(0, rows, rr):
                            most = jnp.maximum(most, block[r:r + rr])
                    return most
                most = lax.fori_loop(0, nz, step, most)
    most = jnp.max(most.astype(F32), axis=0, keepdims=True)
    most = jnp.max(most, axis=1, keepdims=True)
    lim[0] = jnp.broadcast_to(jnp.maximum(most, TINY), (rr, cw))
    to_core = remote(lim.at[0], lim_c, ms.at[0], mr.at[0], c_peer)
    for k in order[lead:]:
        give(k)
    to_core.wait_recv()
    lim[1] = lim[0] + lim_c[...]
    remote(lim.at[1], lim_1.at[0], ms.at[1], mr.at[1], x_peer)
    remote(lim.at[1], lim_1.at[1], ms.at[2], mr.at[2], y_peer)

    def limits(stage):
        if stage == "A":
            for o in range(1, nz):
                remote(lim.at[1], lim_z.at[z], vs.at[0], vr.at[0], z_peer(o))
        if stage == "B":
            done(lim_z.at[pl.ds(0, nz - 1)], vr.at[0])
            most = lim[1]
            for o in range(1, nz):
                most = most + lim_z[lax.rem(z + o, nz)]
            lim[6] = most
            for i, peer in enumerate([d_peer, x_peer, y_peer]):
                remote(lim.at[6], lim_w.at[i], vs.at[1], vr.at[1], peer)
        if stage == "C":
            done(lim_w, vr.at[1])
        if stage == "2":
            for kind, peer in enumerate([y_peer, x_peer]):
                done(lim_1.at[kind], mr.at[1 + kind])
                lim[2 + kind] = lim[1] + lim_1[kind]
                remote(lim.at[2 + kind], lim_2.at[kind], ms.at[3 + kind], mr.at[3 + kind], peer)
        if stage == "3":
            for kind in range(2):
                done(lim_2.at[kind], mr.at[3 + kind])
                lim[4 + kind] = lim[2 + kind] + lim_2[kind]
                for o in range(1, nz):
                    remote(lim.at[4 + kind], lim_3.at[kind, z], ns.at[kind], nr.at[kind], z_peer(o))
        if stage == "4":
            for kind in range(2):
                done(lim_3.at[kind, pl.ds(0, nz - 1)], nr.at[kind])

    def up(ref):
        return (TOP / ref)[None]

    def down(ref):
        return (ref * (1.0 / TOP))[None]

    def p1(k):
        pair[k].wait_recv()
        scale = up(lim[1])
        for b in range(2):
            s1a[k, :, b] = encode(mine(k, 0, 1 - x, b), scale)
        ca = remote(s1a.at[k], r1a.at[k], p1s.at[0], p1r.at[0, k], x_peer)
        for a in range(2):
            s1b[k, a] = encode(mine(k, 1, a, 1 - y), scale)
        cb = remote(s1b.at[k], r1b.at[k], p1s.at[1], p1r.at[1, k], y_peer)
        first[k] = (ca, cb)

    def p2(k):
        a, b = first[k]
        a.wait_recv()
        s2[0, k] = encode(mine(k, 0, x, 1 - y) + decode(r1a[k, :, 1 - y], down(lim_1[0])), up(lim[2]))
        ca = remote(s2.at[0, k], r2.at[0, k], p2s.at[0], p2r.at[0, k], y_peer)
        b.wait_recv()
        s2[1, k] = encode(mine(k, 1, 1 - x, y) + decode(r1b[k, 1 - x], down(lim_1[1])), up(lim[3]))
        cb = remote(s2.at[1, k], r2.at[1, k], p2s.at[1], p2r.at[1, k], x_peer)
        second[k] = (ca, cb)

    def p3(k):
        for kind in range(2):
            lanes = pl.ds(kind * cw, cw)
            if kind == 0:
                total = mine(k, 0, x, y) + decode(r1a[k, :, y], down(lim_1[0]))
            else:
                total = mine(k, 1, x, y) + decode(r1b[k, x], down(lim_1[1]))
            second[k][kind].wait_recv()
            total = total + decode(r2[kind, k], down(lim_2[kind]))
            s3f[k, :, :, lanes] = total
            s3[k, :, :, lanes] = encode(total, up(lim[4 + kind]))
        copies = []
        for o in range(1, nz):
            to = lax.rem(z + o, nz)
            copies.append(remote(s3.at[k, to], r4.at[k, z], p3s.at[0], p3r.at[k], z_peer(o)))
        third[k] = copies

    def z1(i):
        k = steps + i
        pair[k].wait_recv()
        scale = jnp.concatenate([up(lim[1])] * 2, axis=-1)
        d, r, w = span(k)
        for o in range(1, nz):
            to = lax.rem(z + o, nz)
            for a in range(2):
                sz[i, to, a] = encode(own[a, c, d, to, :, r, w].astype(F32) + rp[k, a, to].astype(F32), scale)
            remote(sz.at[i, to], rz.at[i, z], zs.at[0], zr.at[i], z_peer(o))

    def z2(i):
        k = steps + i
        done(rz.at[i, pl.ds(0, nz - 1)], zr.at[i])
        d, r, w = span(k)
        scale = jnp.concatenate([up(lim[6])] * 2, axis=-1)
        for a in range(2):
            total = own[a, c, d, z, :, r, w].astype(F32) + rp[k, a, z].astype(F32)
            for o in range(1, nz):
                of = lax.rem(z + o, nz)
                total = total + decode(rz[i, of, a], jnp.concatenate([down(lim_z[of])] * 2, axis=-1))
            tz[i, a] = total
            sw[i, a] = encode(total, scale)
        for n, (a, b, peer) in enumerate([(1 - x, 1 - y, d_peer), (1 - x, y, x_peer), (x, 1 - y, y_peer)]):
            remote(sw.at[i, a, b], rw.at[i, n], ws.at[0], wr.at[i], peer)

    def z3(i):
        done(rw.at[i], wr.at[i])
        total = tz[i, x, y]
        for n in range(3):
            total = total + decode(rw[i, n], jnp.concatenate([lim_w[n] * (1.0 / TOP)] * 2, axis=-1))
        _, r, w = span(steps + i)
        img[units[steps + i][1], r, w] = total * shrink
        edges(steps + i)

    shrink = 1.0 / jnp.sqrt(F32(groups * members))

    def halo(side, a, b):
        there, peer = beside[side]

        @pl.when(there)
        def _():
            remote(a, b, hs.at[side], hr.at[side], peer)

    def last(k):
        j, d, h = units[k]
        _, r, w = span(k)
        done(r4.at[k, pl.ds(0, nz - 1)], p3r.at[k])
        for kind in range(2):
            lanes = pl.ds(kind * cw, cw)
            total = s3f[k, z, :, lanes]
            for o in range(1, nz):
                at = lax.rem(z + nz - o, nz)
                total = total + decode(r4[k, at, :, lanes], lim_3[kind, at] * (1.0 / TOP))
            img[d, r, kind_cols(kind, k)] = total * shrink
        edges(k)

    def edges(k):
        j, d, h = units[k]
        _, r, w = span(k)
        if d == 0:
            halo(0, img.at[d, r, w], high.at[r, w])
        if d == nd - 1:
            halo(1, img.at[d, r, w], low.at[r, w])
        if h == 0:
            halo(2, img.at[d, pl.ds(0, edge), w], bottom.at[d, :, w])
        if h + rr == rows:
            halo(3, img.at[d, pl.ds(rows - edge, edge), w], top.at[d, :, w])

    def greet():
        for way, (there, peer) in enumerate([near[1], near[0]]):
            behind = z if way == 0 else nz - 1 - z

            @pl.when(behind > 1)
            def _():
                pl.semaphore_wait(chain.at[way], 1)

            @pl.when(jnp.logical_and(there, behind > 0))
            def _():
                pl.semaphore_signal(chain.at[way], inc=1, device_id=peer, device_id_type=MESH)

    run = {"1": p1, "2": p2, "3": p3, "4": last, "A": z1, "B": z2, "C": z3}
    begun = set()
    for op, k in plan(steps, early):
        if op not in begun:
            begun.add(op)
            if op in "A3" and "greet" not in begun:
                begun.add("greet")
                greet()
            limits(op)
        run[op](k)
    rown = lax.broadcasted_iota(jnp.int32, (rows, width), 0)
    coln = lax.broadcasted_iota(jnp.int32, (rows, width), 1)

    def arrive(sides):
        for side in sides:
            @pl.when(beside[side ^ 1][0])
            def _():
                done([high, low, bottom, top][side], hr.at[side])

    arrive([2, 3])
    for d in range(nd):
        here = img[d]
        before = jnp.where(t > 0, top[d, edge - 1:edge, :], 0.0)
        after = jnp.where(t < members - 1, bottom[d, 0:1, :], 0.0)
        near = jnp.where(rown == rows - 1, after, pltpu.roll(here, rows - 1, 0))
        near = near + jnp.where(rown == 0, before, pltpu.roll(here, 1, 0))
        near = near + jnp.where(coln == width - 1, 0.0, pltpu.roll(here, width - 1, 1))
        near = near + jnp.where(coln == 0, 0.0, pltpu.roll(here, 1, 1))
        if d > 0:
            near = near + img[d - 1]
        if d < nd - 1:
            near = near + img[d + 1]
        out[d] = 6.0 * here - near
    arrive([0, 1])
    out[0] = out[0] - jnp.where(g > 0, low[...], 0.0)
    out[nd - 1] = out[nd - 1] - jnp.where(g < groups - 1, high[...], 0.0)
    for side, ref in enumerate([high, low, bottom, top]):
        @pl.when(beside[side][0])
        def _():
            done(ref, hs.at[side])
    done(rp, cs.at[0])
    done(r1a, p1s.at[0])
    done(r1b, p1s.at[1])
    for kind in range(2):
        done(r2.at[kind], p2s.at[kind])
        done(lim_3.at[kind, pl.ds(0, nz - 1)], ns.at[kind])
    done(r4.at[:, pl.ds(0, nz - 1)], p3s.at[0])
    if early:
        done(rz.at[:, pl.ds(0, nz - 1)], zs.at[0])
        done(rw, ws.at[0])
        done(lim_z.at[pl.ds(0, nz - 1)], vs.at[0])
        done(lim_w, vs.at[1])
    for i in range(5):
        done(lim_c, ms.at[i])


def body(groups, members, partials):
    shots, depth, lateral, width = partials.shape
    nd, nz, rows, cw = depth // groups, members // 2, lateral // members, width // 4
    parts = 4 if rows % 64 == 0 else 1
    rr, edge = rows // parts, min(8, rows)
    early = 3 if parts > 1 else 1
    total = 2 * nd * parts
    steps = total - early
    src = partials.reshape(2, 2, nd, nz, 2, rows, width)
    kind = partials.dtype
    dma = pltpu.SemaphoreType.DMA
    return pl.pallas_call(
        functools.partial(kernel, groups, members),
        out_shape=jax.ShapeDtypeStruct((nd, rows, width), F32),
        in_specs=[pl.BlockSpec(memory_space=pl.ANY)],
        out_specs=pl.BlockSpec(memory_space=pltpu.VMEM),
        scratch_shapes=[
            pltpu.VMEM((2, 2, nd, nz, 2, rows, width), kind),
            pltpu.VMEM((total, 2, nz, 2, rr, 2 * cw), kind),
            pltpu.VMEM((steps, nz, 2, rr, cw), kind),
            pltpu.VMEM((steps, 2, nz, rr, cw), kind),
            pltpu.VMEM((steps, nz, 2, rr, cw), kind),
            pltpu.VMEM((steps, 2, nz, rr, cw), kind),
            pltpu.VMEM((2, steps, nz, rr, cw), kind),
            pltpu.VMEM((2, steps, nz, rr, cw), kind),
            pltpu.VMEM((steps, nz, rr, 2 * cw), F32),
            pltpu.VMEM((steps, nz, rr, 2 * cw), kind),
            pltpu.VMEM((steps, nz, rr, 2 * cw), kind),
            pltpu.VMEM((early, nz, 2, 2, rr, 2 * cw), kind),
            pltpu.VMEM((early, nz, 2, 2, rr, 2 * cw), kind),
            pltpu.VMEM((early, 2, 2, rr, 2 * cw), F32),
            pltpu.VMEM((early, 2, 2, rr, 2 * cw), kind),
            pltpu.VMEM((early, 3, rr, 2 * cw), kind),
            pltpu.VMEM((7, rr, cw), F32),
            pltpu.VMEM((rr, cw), F32),
            pltpu.VMEM((2, rr, cw), F32),
            pltpu.VMEM((2, rr, cw), F32),
            pltpu.VMEM((2, nz, rr, cw), F32),
            pltpu.VMEM((nz, rr, cw), F32),
            pltpu.VMEM((3, rr, cw), F32),
            pltpu.VMEM((nd, rows, width), F32),
            pltpu.VMEM((rows, width), F32),
            pltpu.VMEM((rows, width), F32),
            pltpu.VMEM((nd, edge, width), F32),
            pltpu.VMEM((nd, edge, width), F32),
            dma((2 * nd,)),
            dma((1,)), dma((total,)),
            dma((2,)), dma((2, steps)),
            dma((2,)), dma((2, steps)),
            dma((1,)), dma((steps,)),
            dma((1,)), dma((early,)),
            dma((1,)), dma((early,)),
            dma((5,)), dma((5,)),
            dma((2,)), dma((2,)),
            dma((2,)), dma((2,)),
            dma((4,)), dma((4,)),
            pltpu.SemaphoreType.REGULAR((2,)),
        ],
        compiler_params=pltpu.CompilerParams(collective_id=0, has_side_effects=True, vmem_limit_bytes=51 * 2**20),
    )(src)


def solution(mesh):
    groups, members = mesh.shape["shot"], mesh.shape["tile"]
    return jax.shard_map(
        functools.partial(body, groups, members),
        mesh=mesh,
        in_specs=(P(("shot", "tile"), None, None, None),),
        out_specs=P("shot", "tile", None),
        check_vma=False,
    )
```

```python
import functools

import jax
import jax.numpy as jnp
from jax import lax
from jax.experimental import pallas as pl
from jax.experimental.pallas import tpu as pltpu
from jax.sharding import PartitionSpec as P

MESH = pl.DeviceIdType.MESH
F32 = jnp.float32
TOP = 180.0
TINY = 1e-30


def plan(steps, early):
    ahead, lag, single, least, before, at_b = 5, 6, 0, 4, 2, 11
    ahead = min(ahead, steps)
    third = [max(k + least, lag + min(k, single) + max(k - single, 0) // 2) for k in range(steps)]
    seq = []
    for k in range(ahead):
        seq.append(("1", k))
        if 1 <= k <= early:
            seq.append(("A", k - 1))
    seq += [("A", k) for k in range(max(ahead - 1, 0), early)]
    ends = list(range(steps))
    for k in range(third[-1] + 1):
        if k < steps:
            seq.append(("2", k))
        if k + ahead < steps:
            seq.append(("1", k + ahead))
        if k == min(at_b, steps - 1):
            seq += [("B", i) for i in range(early)]
        seq += [("3", i) for i in range(steps) if third[i] == k]
        if third[-1] - before <= k < third[-1] and third[ends[0]] < k:
            seq.append(("4", ends.pop(0)))
    for i in ends:
        if i == ends[-2 if len(ends) > 1 else -1]:
            seq += [("C", j) for j in range(early)]
        seq.append(("4", i))
    return seq


def encode(value, scale):
    w = value * scale
    p = w * w
    p = p * p
    p = p * p
    p = p * p
    return jnp.where(w < 0.0, -p, p).astype(jnp.bfloat16)


def decode(code, scale):
    code = code.astype(F32)
    root = lax.rsqrt(lax.rsqrt(lax.rsqrt(lax.rsqrt(jnp.abs(code))))) * scale
    return jnp.where(code < 0.0, -root, root)


def kernel(groups, members, src, out, own, rp, s1a, s1b, r1a, r1b, s2, r2, s3f, s3, r4,
           sz, rz, tz, sw, rw, lim, lim_c, lim_1, lim_2, lim_3, lim_z, lim_w,
           img, low, high, top, bottom, own_sem, cs, cr, p1s, p1r, p2s, p2r, p3s, p3r,
           zs, zr, ws, wr, ms, mr, ns, nr, vs, vr, hs, hr, chain):
    nd, nz, rows, width = src.shape[2], src.shape[3], src.shape[5], src.shape[6]
    cw = width // 4
    rr = s2.shape[3]
    edge = top.shape[1]
    units = [(j, d, h) for d in range(nd) for h in range(0, rows, rr) for j in range(2)]
    early = sz.shape[0]
    at = len(units) * 5 // 8
    late = units[at:at + early]
    units = units[:at] + units[at + early:] + late
    total_steps = len(units)
    steps = total_steps - early
    g, t = lax.axis_index("shot"), lax.axis_index("tile")
    x, c = g // 2, g % 2
    z, y = t // 2, t % 2

    def dev(gx, tx):
        return {"shot": gx, "tile": tx}

    x_peer = dev((1 - x) * 2 + c, t)
    c_peer = dev(x * 2 + 1 - c, t)
    y_peer = dev(g, z * 2 + 1 - y)
    d_peer = dev((1 - x) * 2 + c, z * 2 + 1 - y)

    def z_peer(o):
        return dev(g, lax.rem(z + o, nz) * 2 + y)

    beside = [
        (g > 0, dev(g - 1, t)),
        (g < groups - 1, dev(g + 1, t)),
        (t > 0, dev(g, t - 1)),
        (t < members - 1, dev(g, t + 1)),
    ]

    barrier = pltpu.get_barrier_semaphore()
    near = [(z > 0, dev(g, t - 2)), (z < nz - 1, dev(g, t + 2))]
    peers = [c_peer, x_peer, y_peer]
    count = jnp.int32(len(peers))
    for peer in peers:
        pl.semaphore_signal(barrier, inc=1, device_id=peer, device_id_type=MESH)
    for there, peer in near:
        count = count + jnp.where(there, 1, 0)

        @pl.when(there)
        def _():
            pl.semaphore_signal(barrier, inc=1, device_id=peer, device_id_type=MESH)
    loads = []
    for d in range(nd):
        for core in range(2):
            i = 2 * d + core
            at = 1 - c if core == 0 else c
            loads.append(pltpu.make_async_copy(src.at[:, at, d], own.at[:, at, d], own_sem.at[i]))
    for copy in loads:
        copy.start()

    def remote(a, b, s, r, peer):
        copy = pltpu.make_async_remote_copy(
            src_ref=a, dst_ref=b, send_sem=s, recv_sem=r, device_id=peer, device_id_type=MESH
        )
        copy.start()
        return copy

    def done(ref, sem):
        pltpu.make_async_copy(ref, ref, sem).wait()

    pair, first, second, third = {}, {}, {}, {}

    def span(k):
        j, d, h = units[k]
        return d, pl.ds(h, rr), pl.ds(2 * j * cw, 2 * cw)

    def kind_cols(kind, k):
        j, d, h = units[k]
        return pl.ds((2 * j + kind) * cw, cw)

    def give(k):
        d, r, w = span(k)
        pair[k] = remote(own.at[:, 1 - c, d, :, :, r, w], rp.at[k], cs.at[0], cr.at[k], c_peer)

    def mine(k, kind, a, b):
        d, r, _ = span(k)
        lanes = pl.ds(kind * cw, cw)
        return own[a, c, d, :, b, r, kind_cols(kind, k)].astype(F32) + rp[k, a, :, b, :, lanes].astype(F32)

    order = []
    for k in range(steps):
        order.append(k)
        if 1 <= k <= early:
            order.append(steps + k - 1)
    lead = 2
    most = jnp.zeros((rr, width), own.dtype)
    for d in range(nd):
        for core in range(2):
            loads[2 * d + core].wait()
            if d == 0 and core == 0:
                pl.semaphore_wait(barrier, count)
                for k in order[:lead]:
                    give(k)
            at = 1 - c if core == 0 else c
            for a in range(2):
                def step(i, most, a=a, at=at, d=d):
                    for b in range(2):
                        block = jnp.abs(own[a, at, d, i, b])
                        for r in range(0, rows, rr):
                            most = jnp.maximum(most, block[r:r + rr])
                    return most
                most = lax.fori_loop(0, nz, step, most)
    most = jnp.max(most.astype(F32), axis=0, keepdims=True)
    most = jnp.max(most, axis=1, keepdims=True)
    lim[0] = jnp.broadcast_to(jnp.maximum(most, TINY), (rr, cw))
    to_core = remote(lim.at[0], lim_c, ms.at[0], mr.at[0], c_peer)
    for k in order[lead:]:
        give(k)
    to_core.wait_recv()
    lim[1] = lim[0] + lim_c[...]
    remote(lim.at[1], lim_1.at[0], ms.at[1], mr.at[1], x_peer)
    remote(lim.at[1], lim_1.at[1], ms.at[2], mr.at[2], y_peer)

    def limits(stage):
        if stage == "A":
            for o in range(1, nz):
                remote(lim.at[1], lim_z.at[z], vs.at[0], vr.at[0], z_peer(o))
        if stage == "B":
            done(lim_z.at[pl.ds(0, nz - 1)], vr.at[0])
            most = lim[1]
            for o in range(1, nz):
                most = most + lim_z[lax.rem(z + o, nz)]
            lim[6] = most
            for i, peer in enumerate([d_peer, x_peer, y_peer]):
                remote(lim.at[6], lim_w.at[i], vs.at[1], vr.at[1], peer)
        if stage == "C":
            done(lim_w, vr.at[1])
        if stage == "2":
            for kind, peer in enumerate([y_peer, x_peer]):
                done(lim_1.at[kind], mr.at[1 + kind])
                lim[2 + kind] = lim[1] + lim_1[kind]
                remote(lim.at[2 + kind], lim_2.at[kind], ms.at[3 + kind], mr.at[3 + kind], peer)
        if stage == "3":
            for kind in range(2):
                done(lim_2.at[kind], mr.at[3 + kind])
                lim[4 + kind] = lim[2 + kind] + lim_2[kind]
                for o in range(1, nz):
                    remote(lim.at[4 + kind], lim_3.at[kind, z], ns.at[kind], nr.at[kind], z_peer(o))
        if stage == "4":
            for kind in range(2):
                done(lim_3.at[kind, pl.ds(0, nz - 1)], nr.at[kind])

    def up(ref):
        return (TOP / ref)[None]

    def down(ref):
        return (ref * (1.0 / TOP))[None]

    def p1(k):
        pair[k].wait_recv()
        scale = up(lim[1])
        for b in range(2):
            s1a[k, :, b] = encode(mine(k, 0, 1 - x, b), scale)
        ca = remote(s1a.at[k], r1a.at[k], p1s.at[0], p1r.at[0, k], x_peer)
        for a in range(2):
            s1b[k, a] = encode(mine(k, 1, a, 1 - y), scale)
        cb = remote(s1b.at[k], r1b.at[k], p1s.at[1], p1r.at[1, k], y_peer)
        first[k] = (ca, cb)

    def p2(k):
        a, b = first[k]
        a.wait_recv()
        s2[0, k] = encode(mine(k, 0, x, 1 - y) + decode(r1a[k, :, 1 - y], down(lim_1[0])), up(lim[2]))
        ca = remote(s2.at[0, k], r2.at[0, k], p2s.at[0], p2r.at[0, k], y_peer)
        b.wait_recv()
        s2[1, k] = encode(mine(k, 1, 1 - x, y) + decode(r1b[k, 1 - x], down(lim_1[1])), up(lim[3]))
        cb = remote(s2.at[1, k], r2.at[1, k], p2s.at[1], p2r.at[1, k], x_peer)
        second[k] = (ca, cb)

    def p3(k):
        for kind in range(2):
            lanes = pl.ds(kind * cw, cw)
            if kind == 0:
                total = mine(k, 0, x, y) + decode(r1a[k, :, y], down(lim_1[0]))
            else:
                total = mine(k, 1, x, y) + decode(r1b[k, x], down(lim_1[1]))
            second[k][kind].wait_recv()
            total = total + decode(r2[kind, k], down(lim_2[kind]))
            s3f[k, :, :, lanes] = total
            s3[k, :, :, lanes] = encode(total, up(lim[4 + kind]))
        copies = []
        for o in range(1, nz):
            to = lax.rem(z + o, nz)
            copies.append(remote(s3.at[k, to], r4.at[k, z], p3s.at[0], p3r.at[k], z_peer(o)))
        third[k] = copies

    def z1(i):
        k = steps + i
        pair[k].wait_recv()
        scale = jnp.concatenate([up(lim[1])] * 2, axis=-1)
        d, r, w = span(k)
        for o in range(1, nz):
            to = lax.rem(z + o, nz)
            for a in range(2):
                sz[i, to, a] = encode(own[a, c, d, to, :, r, w].astype(F32) + rp[k, a, to].astype(F32), scale)
            remote(sz.at[i, to], rz.at[i, z], zs.at[0], zr.at[i], z_peer(o))

    def z2(i):
        k = steps + i
        done(rz.at[i, pl.ds(0, nz - 1)], zr.at[i])
        d, r, w = span(k)
        scale = jnp.concatenate([up(lim[6])] * 2, axis=-1)
        for a in range(2):
            total = own[a, c, d, z, :, r, w].astype(F32) + rp[k, a, z].astype(F32)
            for o in range(1, nz):
                of = lax.rem(z + o, nz)
                total = total + decode(rz[i, of, a], jnp.concatenate([down(lim_z[of])] * 2, axis=-1))
            tz[i, a] = total
            sw[i, a] = encode(total, scale)
        for n, (a, b, peer) in enumerate([(1 - x, 1 - y, d_peer), (1 - x, y, x_peer), (x, 1 - y, y_peer)]):
            remote(sw.at[i, a, b], rw.at[i, n], ws.at[0], wr.at[i], peer)

    def z3(i):
        done(rw.at[i], wr.at[i])
        total = tz[i, x, y]
        for n in range(3):
            total = total + decode(rw[i, n], jnp.concatenate([lim_w[n] * (1.0 / TOP)] * 2, axis=-1))
        _, r, w = span(steps + i)
        img[units[steps + i][1], r, w] = total * shrink
        edges(steps + i)

    shrink = 1.0 / jnp.sqrt(F32(groups * members))

    def halo(side, a, b):
        there, peer = beside[side]

        @pl.when(there)
        def _():
            remote(a, b, hs.at[side], hr.at[side], peer)

    def last(k):
        j, d, h = units[k]
        _, r, w = span(k)
        done(r4.at[k, pl.ds(0, nz - 1)], p3r.at[k])
        for kind in range(2):
            lanes = pl.ds(kind * cw, cw)
            total = s3f[k, z, :, lanes]
            for o in range(1, nz):
                at = lax.rem(z + nz - o, nz)
                total = total + decode(r4[k, at, :, lanes], lim_3[kind, at] * (1.0 / TOP))
            img[d, r, kind_cols(kind, k)] = total * shrink
        edges(k)

    def edges(k):
        j, d, h = units[k]
        _, r, w = span(k)
        if d == 0:
            halo(0, img.at[d, r, w], high.at[r, w])
        if d == nd - 1:
            halo(1, img.at[d, r, w], low.at[r, w])
        if h == 0:
            halo(2, img.at[d, pl.ds(0, edge), w], bottom.at[d, :, w])
        if h + rr == rows:
            halo(3, img.at[d, pl.ds(rows - edge, edge), w], top.at[d, :, w])

    def greet():
        for way, (there, peer) in enumerate([near[1], near[0]]):
            behind = z if way == 0 else nz - 1 - z

            @pl.when(behind > 1)
            def _():
                pl.semaphore_wait(chain.at[way], 1)

            @pl.when(jnp.logical_and(there, behind > 0))
            def _():
                pl.semaphore_signal(chain.at[way], inc=1, device_id=peer, device_id_type=MESH)

    run = {"1": p1, "2": p2, "3": p3, "4": last, "A": z1, "B": z2, "C": z3}
    begun = set()
    for op, k in plan(steps, early):
        if op not in begun:
            begun.add(op)
            if op in "A3" and "greet" not in begun:
                begun.add("greet")
                greet()
            limits(op)
        run[op](k)
    rown = lax.broadcasted_iota(jnp.int32, (rows, width), 0)
    coln = lax.broadcasted_iota(jnp.int32, (rows, width), 1)

    def arrive(sides):
        for side in sides:
            @pl.when(beside[side ^ 1][0])
            def _():
                done([high, low, bottom, top][side], hr.at[side])

    arrive([2, 3])
    for d in range(nd):
        here = img[d]
        before = jnp.where(t > 0, top[d, edge - 1:edge, :], 0.0)
        after = jnp.where(t < members - 1, bottom[d, 0:1, :], 0.0)
        near = jnp.where(rown == rows - 1, after, pltpu.roll(here, rows - 1, 0))
        near = near + jnp.where(rown == 0, before, pltpu.roll(here, 1, 0))
        near = near + jnp.where(coln == width - 1, 0.0, pltpu.roll(here, width - 1, 1))
        near = near + jnp.where(coln == 0, 0.0, pltpu.roll(here, 1, 1))
        if d > 0:
            near = near + img[d - 1]
        if d < nd - 1:
            near = near + img[d + 1]
        out[d] = 6.0 * here - near
    arrive([0, 1])
    out[0] = out[0] - jnp.where(g > 0, low[...], 0.0)
    out[nd - 1] = out[nd - 1] - jnp.where(g < groups - 1, high[...], 0.0)
    for side, ref in enumerate([high, low, bottom, top]):
        @pl.when(beside[side][0])
        def _():
            done(ref, hs.at[side])
    done(rp, cs.at[0])
    done(r1a, p1s.at[0])
    done(r1b, p1s.at[1])
    for kind in range(2):
        done(r2.at[kind], p2s.at[kind])
        done(lim_3.at[kind, pl.ds(0, nz - 1)], ns.at[kind])
    done(r4.at[:, pl.ds(0, nz - 1)], p3s.at[0])
    if early:
        done(rz.at[:, pl.ds(0, nz - 1)], zs.at[0])
        done(rw, ws.at[0])
        done(lim_z.at[pl.ds(0, nz - 1)], vs.at[0])
        done(lim_w, vs.at[1])
    for i in range(5):
        done(lim_c, ms.at[i])


def body(groups, members, partials):
    shots, depth, lateral, width = partials.shape
    nd, nz, rows, cw = depth // groups, members // 2, lateral // members, width // 4
    parts = 4 if rows % 64 == 0 else 1
    rr, edge = rows // parts, min(8, rows)
    early = 2 if parts > 1 else 1
    total = 2 * nd * parts
    steps = total - early
    src = partials.reshape(2, 2, nd, nz, 2, rows, width)
    kind = partials.dtype
    dma = pltpu.SemaphoreType.DMA
    return pl.pallas_call(
        functools.partial(kernel, groups, members),
        out_shape=jax.ShapeDtypeStruct((nd, rows, width), F32),
        in_specs=[pl.BlockSpec(memory_space=pl.ANY)],
        out_specs=pl.BlockSpec(memory_space=pltpu.VMEM),
        scratch_shapes=[
            pltpu.VMEM((2, 2, nd, nz, 2, rows, width), kind),
            pltpu.VMEM((total, 2, nz, 2, rr, 2 * cw), kind),
            pltpu.VMEM((steps, nz, 2, rr, cw), kind),
            pltpu.VMEM((steps, 2, nz, rr, cw), kind),
            pltpu.VMEM((steps, nz, 2, rr, cw), kind),
            pltpu.VMEM((steps, 2, nz, rr, cw), kind),
            pltpu.VMEM((2, steps, nz, rr, cw), kind),
            pltpu.VMEM((2, steps, nz, rr, cw), kind),
            pltpu.VMEM((steps, nz, rr, 2 * cw), F32),
            pltpu.VMEM((steps, nz, rr, 2 * cw), kind),
            pltpu.VMEM((steps, nz, rr, 2 * cw), kind),
            pltpu.VMEM((early, nz, 2, 2, rr, 2 * cw), kind),
            pltpu.VMEM((early, nz, 2, 2, rr, 2 * cw), kind),
            pltpu.VMEM((early, 2, 2, rr, 2 * cw), F32),
            pltpu.VMEM((early, 2, 2, rr, 2 * cw), kind),
            pltpu.VMEM((early, 3, rr, 2 * cw), kind),
            pltpu.VMEM((7, rr, cw), F32),
            pltpu.VMEM((rr, cw), F32),
            pltpu.VMEM((2, rr, cw), F32),
            pltpu.VMEM((2, rr, cw), F32),
            pltpu.VMEM((2, nz, rr, cw), F32),
            pltpu.VMEM((nz, rr, cw), F32),
            pltpu.VMEM((3, rr, cw), F32),
            pltpu.VMEM((nd, rows, width), F32),
            pltpu.VMEM((rows, width), F32),
            pltpu.VMEM((rows, width), F32),
            pltpu.VMEM((nd, edge, width), F32),
            pltpu.VMEM((nd, edge, width), F32),
            dma((2 * nd,)),
            dma((1,)), dma((total,)),
            dma((2,)), dma((2, steps)),
            dma((2,)), dma((2, steps)),
            dma((1,)), dma((steps,)),
            dma((1,)), dma((early,)),
            dma((1,)), dma((early,)),
            dma((5,)), dma((5,)),
            dma((2,)), dma((2,)),
            dma((2,)), dma((2,)),
            dma((4,)), dma((4,)),
            pltpu.SemaphoreType.REGULAR((2,)),
        ],
        compiler_params=pltpu.CompilerParams(collective_id=0, has_side_effects=True, vmem_limit_bytes=51 * 2**20),
    )(src)


def solution(mesh):
    groups, members = mesh.shape["shot"], mesh.shape["tile"]
    return jax.shard_map(
        functools.partial(body, groups, members),
        mesh=mesh,
        in_specs=(P(("shot", "tile"), None, None, None),),
        out_specs=P("shot", "tile", None),
        check_vma=False,
    )
```

```python
import functools

import jax
import jax.numpy as jnp
from jax import lax
from jax.experimental import pallas as pl
from jax.experimental.pallas import tpu as pltpu
from jax.sharding import PartitionSpec as P

MESH = pl.DeviceIdType.MESH
F32 = jnp.float32
TOP = 180.0
TINY = 1e-30


def plan(steps, early):
    ahead, lag, single, least, before, at_b = 5, 6, 0, 4, 2, 11
    ahead = min(ahead, steps)
    third = [max(k + least, lag + min(k, single) + max(k - single, 0) // 2) for k in range(steps)]
    seq = []
    for k in range(ahead):
        seq.append(("1", k))
        if 1 <= k <= early:
            seq.append(("A", k - 1))
    seq += [("A", k) for k in range(max(ahead - 1, 0), early)]
    ends = list(range(steps))
    for k in range(third[-1] + 1):
        if k < steps:
            seq.append(("2", k))
        if k + ahead < steps:
            seq.append(("1", k + ahead))
        if k == min(at_b, steps - 1):
            seq += [("B", i) for i in range(early)]
        seq += [("3", i) for i in range(steps) if third[i] == k]
        if third[-1] - before <= k < third[-1] and third[ends[0]] < k:
            seq.append(("4", ends.pop(0)))
    for i in ends:
        if i == ends[-2 if len(ends) > 1 else -1]:
            seq += [("C", j) for j in range(early)]
        seq.append(("4", i))
    return seq


def encode(value, scale):
    w = value * scale
    p = w * w
    p = p * p
    p = p * p
    p = p * p
    return jnp.where(w < 0.0, -p, p).astype(jnp.bfloat16)


def decode(code, scale):
    code = code.astype(F32)
    root = lax.rsqrt(lax.rsqrt(lax.rsqrt(lax.rsqrt(jnp.abs(code))))) * scale
    return jnp.where(code < 0.0, -root, root)


def kernel(groups, members, src, out, own, rp, s1a, s1b, r1a, r1b, s2, r2, s3f, s3, r4,
           sz, rz, tz, sw, rw, lim, lim_c, lim_1, lim_2, lim_3, lim_z, lim_w,
           img, low, high, top, bottom, own_sem, cs, cr, p1s, p1r, p2s, p2r, p3s, p3r,
           zs, zr, ws, wr, ms, mr, ns, nr, vs, vr, hs, hr, chain):
    nd, nz, rows, width = src.shape[2], src.shape[3], src.shape[5], src.shape[6]
    cw = width // 4
    rr = s2.shape[3]
    edge = top.shape[1]
    units = [(j, d, h) for d in range(nd) for h in range(0, rows, rr) for j in range(2)]
    units = sorted(units, key=lambda unit: 0 < unit[2] < rows - rr)
    early = sz.shape[0]
    at = len(units) * 5 // 8
    late = units[at:at + early]
    units = units[:at] + units[at + early:] + late
    total_steps = len(units)
    steps = total_steps - early
    g, t = lax.axis_index("shot"), lax.axis_index("tile")
    x, c = g // 2, g % 2
    z, y = t // 2, t % 2

    def dev(gx, tx):
        return {"shot": gx, "tile": tx}

    x_peer = dev((1 - x) * 2 + c, t)
    c_peer = dev(x * 2 + 1 - c, t)
    y_peer = dev(g, z * 2 + 1 - y)
    d_peer = dev((1 - x) * 2 + c, z * 2 + 1 - y)

    def z_peer(o):
        return dev(g, lax.rem(z + o, nz) * 2 + y)

    beside = [
        (g > 0, dev(g - 1, t)),
        (g < groups - 1, dev(g + 1, t)),
        (t > 0, dev(g, t - 1)),
        (t < members - 1, dev(g, t + 1)),
    ]

    barrier = pltpu.get_barrier_semaphore()
    near = [(z > 0, dev(g, t - 2)), (z < nz - 1, dev(g, t + 2))]
    peers = [c_peer, x_peer, y_peer]
    count = jnp.int32(len(peers))
    for peer in peers:
        pl.semaphore_signal(barrier, inc=1, device_id=peer, device_id_type=MESH)
    for there, peer in near:
        count = count + jnp.where(there, 1, 0)

        @pl.when(there)
        def _():
            pl.semaphore_signal(barrier, inc=1, device_id=peer, device_id_type=MESH)
    loads = []
    for d in range(nd):
        for core in range(2):
            i = 2 * d + core
            at = 1 - c if core == 0 else c
            loads.append(pltpu.make_async_copy(src.at[:, at, d], own.at[:, at, d], own_sem.at[i]))
    for copy in loads:
        copy.start()

    def remote(a, b, s, r, peer):
        copy = pltpu.make_async_remote_copy(
            src_ref=a, dst_ref=b, send_sem=s, recv_sem=r, device_id=peer, device_id_type=MESH
        )
        copy.start()
        return copy

    def done(ref, sem):
        pltpu.make_async_copy(ref, ref, sem).wait()

    pair, first, second, third = {}, {}, {}, {}

    def span(k):
        j, d, h = units[k]
        return d, pl.ds(h, rr), pl.ds(2 * j * cw, 2 * cw)

    def kind_cols(kind, k):
        j, d, h = units[k]
        return pl.ds((2 * j + kind) * cw, cw)

    def give(k):
        d, r, w = span(k)
        pair[k] = remote(own.at[:, 1 - c, d, :, :, r, w], rp.at[k], cs.at[0], cr.at[k], c_peer)

    def mine(k, kind, a, b):
        d, r, _ = span(k)
        lanes = pl.ds(kind * cw, cw)
        return own[a, c, d, :, b, r, kind_cols(kind, k)].astype(F32) + rp[k, a, :, b, :, lanes].astype(F32)

    order = []
    for k in range(steps):
        order.append(k)
        if 1 <= k <= early:
            order.append(steps + k - 1)
    lead = 2
    most = jnp.zeros((rr, width), own.dtype)
    for d in range(nd):
        for core in range(2):
            loads[2 * d + core].wait()
            if d == 0 and core == 0:
                pl.semaphore_wait(barrier, count)
                for k in order[:lead]:
                    give(k)
            at = 1 - c if core == 0 else c
            for a in range(2):
                def step(i, most, a=a, at=at, d=d):
                    for b in range(2):
                        block = jnp.abs(own[a, at, d, i, b])
                        for r in range(0, rows, rr):
                            most = jnp.maximum(most, block[r:r + rr])
                    return most
                most = lax.fori_loop(0, nz, step, most)
    most = jnp.max(most.astype(F32), axis=0, keepdims=True)
    most = jnp.max(most, axis=1, keepdims=True)
    lim[0] = jnp.broadcast_to(jnp.maximum(most, TINY), (rr, cw))
    to_core = remote(lim.at[0], lim_c, ms.at[0], mr.at[0], c_peer)
    for k in order[lead:]:
        give(k)
    to_core.wait_recv()
    lim[1] = lim[0] + lim_c[...]
    remote(lim.at[1], lim_1.at[0], ms.at[1], mr.at[1], x_peer)
    remote(lim.at[1], lim_1.at[1], ms.at[2], mr.at[2], y_peer)

    def limits(stage):
        if stage == "A":
            for o in range(1, nz):
                remote(lim.at[1], lim_z.at[z], vs.at[0], vr.at[0], z_peer(o))
        if stage == "B":
            done(lim_z.at[pl.ds(0, nz - 1)], vr.at[0])
            most = lim[1]
            for o in range(1, nz):
                most = most + lim_z[lax.rem(z + o, nz)]
            lim[6] = most
            for i, peer in enumerate([d_peer, x_peer, y_peer]):
                remote(lim.at[6], lim_w.at[i], vs.at[1], vr.at[1], peer)
        if stage == "C":
            done(lim_w, vr.at[1])
        if stage == "2":
            for kind, peer in enumerate([y_peer, x_peer]):
                done(lim_1.at[kind], mr.at[1 + kind])
                lim[2 + kind] = lim[1] + lim_1[kind]
                remote(lim.at[2 + kind], lim_2.at[kind], ms.at[3 + kind], mr.at[3 + kind], peer)
        if stage == "3":
            for kind in range(2):
                done(lim_2.at[kind], mr.at[3 + kind])
                lim[4 + kind] = lim[2 + kind] + lim_2[kind]
                for o in range(1, nz):
                    remote(lim.at[4 + kind], lim_3.at[kind, z], ns.at[kind], nr.at[kind], z_peer(o))
        if stage == "4":
            for kind in range(2):
                done(lim_3.at[kind, pl.ds(0, nz - 1)], nr.at[kind])

    def up(ref):
        return (TOP / ref)[None]

    def down(ref):
        return (ref * (1.0 / TOP))[None]

    def p1(k):
        pair[k].wait_recv()
        scale = up(lim[1])
        for b in range(2):
            s1a[k, :, b] = encode(mine(k, 0, 1 - x, b), scale)
        ca = remote(s1a.at[k], r1a.at[k], p1s.at[0], p1r.at[0, k], x_peer)
        for a in range(2):
            s1b[k, a] = encode(mine(k, 1, a, 1 - y), scale)
        cb = remote(s1b.at[k], r1b.at[k], p1s.at[1], p1r.at[1, k], y_peer)
        first[k] = (ca, cb)

    def p2(k):
        a, b = first[k]
        a.wait_recv()
        s2[0, k] = encode(mine(k, 0, x, 1 - y) + decode(r1a[k, :, 1 - y], down(lim_1[0])), up(lim[2]))
        ca = remote(s2.at[0, k], r2.at[0, k], p2s.at[0], p2r.at[0, k], y_peer)
        b.wait_recv()
        s2[1, k] = encode(mine(k, 1, 1 - x, y) + decode(r1b[k, 1 - x], down(lim_1[1])), up(lim[3]))
        cb = remote(s2.at[1, k], r2.at[1, k], p2s.at[1], p2r.at[1, k], x_peer)
        second[k] = (ca, cb)

    def p3(k):
        for kind in range(2):
            lanes = pl.ds(kind * cw, cw)
            if kind == 0:
                total = mine(k, 0, x, y) + decode(r1a[k, :, y], down(lim_1[0]))
            else:
                total = mine(k, 1, x, y) + decode(r1b[k, x], down(lim_1[1]))
            second[k][kind].wait_recv()
            total = total + decode(r2[kind, k], down(lim_2[kind]))
            s3f[k, :, :, lanes] = total
            s3[k, :, :, lanes] = encode(total, up(lim[4 + kind]))
        copies = []
        for o in range(1, nz):
            to = lax.rem(z + o, nz)
            copies.append(remote(s3.at[k, to], r4.at[k, z], p3s.at[0], p3r.at[k], z_peer(o)))
        third[k] = copies

    def z1(i):
        k = steps + i
        pair[k].wait_recv()
        scale = jnp.concatenate([up(lim[1])] * 2, axis=-1)
        d, r, w = span(k)
        for o in range(1, nz):
            to = lax.rem(z + o, nz)
            for a in range(2):
                sz[i, to, a] = encode(own[a, c, d, to, :, r, w].astype(F32) + rp[k, a, to].astype(F32), scale)
            remote(sz.at[i, to], rz.at[i, z], zs.at[0], zr.at[i], z_peer(o))

    def z2(i):
        k = steps + i
        done(rz.at[i, pl.ds(0, nz - 1)], zr.at[i])
        d, r, w = span(k)
        scale = jnp.concatenate([up(lim[6])] * 2, axis=-1)
        for a in range(2):
            total = own[a, c, d, z, :, r, w].astype(F32) + rp[k, a, z].astype(F32)
            for o in range(1, nz):
                of = lax.rem(z + o, nz)
                total = total + decode(rz[i, of, a], jnp.concatenate([down(lim_z[of])] * 2, axis=-1))
            tz[i, a] = total
            sw[i, a] = encode(total, scale)
        for n, (a, b, peer) in enumerate([(1 - x, 1 - y, d_peer), (1 - x, y, x_peer), (x, 1 - y, y_peer)]):
            remote(sw.at[i, a, b], rw.at[i, n], ws.at[0], wr.at[i], peer)

    def z3(i):
        done(rw.at[i], wr.at[i])
        total = tz[i, x, y]
        for n in range(3):
            total = total + decode(rw[i, n], jnp.concatenate([lim_w[n] * (1.0 / TOP)] * 2, axis=-1))
        _, r, w = span(steps + i)
        img[units[steps + i][1], r, w] = total * shrink
        edges(steps + i)

    shrink = 1.0 / jnp.sqrt(F32(groups * members))

    def halo(side, a, b):
        there, peer = beside[side]

        @pl.when(there)
        def _():
            remote(a, b, hs.at[side], hr.at[side], peer)

    def last(k):
        j, d, h = units[k]
        _, r, w = span(k)
        done(r4.at[k, pl.ds(0, nz - 1)], p3r.at[k])
        for kind in range(2):
            lanes = pl.ds(kind * cw, cw)
            total = s3f[k, z, :, lanes]
            for o in range(1, nz):
                at = lax.rem(z + nz - o, nz)
                total = total + decode(r4[k, at, :, lanes], lim_3[kind, at] * (1.0 / TOP))
            img[d, r, kind_cols(kind, k)] = total * shrink
        edges(k)

    def edges(k):
        j, d, h = units[k]
        _, r, w = span(k)
        if d == 0:
            halo(0, img.at[d, r, w], high.at[r, w])
        if d == nd - 1:
            halo(1, img.at[d, r, w], low.at[r, w])
        if h == 0:
            halo(2, img.at[d, pl.ds(0, edge), w], bottom.at[d, :, w])
        if h + rr == rows:
            halo(3, img.at[d, pl.ds(rows - edge, edge), w], top.at[d, :, w])

    def greet():
        for way, (there, peer) in enumerate([near[1], near[0]]):
            behind = z if way == 0 else nz - 1 - z

            @pl.when(behind > 1)
            def _():
                pl.semaphore_wait(chain.at[way], 1)

            @pl.when(jnp.logical_and(there, behind > 0))
            def _():
                pl.semaphore_signal(chain.at[way], inc=1, device_id=peer, device_id_type=MESH)

    run = {"1": p1, "2": p2, "3": p3, "4": last, "A": z1, "B": z2, "C": z3}
    begun = set()
    for op, k in plan(steps, early):
        if op not in begun:
            begun.add(op)
            if op in "A3" and "greet" not in begun:
                begun.add("greet")
                greet()
            limits(op)
        run[op](k)
    rown = lax.broadcasted_iota(jnp.int32, (rows, width), 0)
    coln = lax.broadcasted_iota(jnp.int32, (rows, width), 1)

    def arrive(sides):
        for side in sides:
            @pl.when(beside[side ^ 1][0])
            def _():
                done([high, low, bottom, top][side], hr.at[side])

    arrive([2, 3])
    for d in range(nd):
        here = img[d]
        before = jnp.where(t > 0, top[d, edge - 1:edge, :], 0.0)
        after = jnp.where(t < members - 1, bottom[d, 0:1, :], 0.0)
        near = jnp.where(rown == rows - 1, after, pltpu.roll(here, rows - 1, 0))
        near = near + jnp.where(rown == 0, before, pltpu.roll(here, 1, 0))
        near = near + jnp.where(coln == width - 1, 0.0, pltpu.roll(here, width - 1, 1))
        near = near + jnp.where(coln == 0, 0.0, pltpu.roll(here, 1, 1))
        if d > 0:
            near = near + img[d - 1]
        if d < nd - 1:
            near = near + img[d + 1]
        out[d] = 6.0 * here - near
    arrive([0, 1])
    out[0] = out[0] - jnp.where(g > 0, low[...], 0.0)
    out[nd - 1] = out[nd - 1] - jnp.where(g < groups - 1, high[...], 0.0)
    for side, ref in enumerate([high, low, bottom, top]):
        @pl.when(beside[side][0])
        def _():
            done(ref, hs.at[side])
    done(rp, cs.at[0])
    done(r1a, p1s.at[0])
    done(r1b, p1s.at[1])
    for kind in range(2):
        done(r2.at[kind], p2s.at[kind])
        done(lim_3.at[kind, pl.ds(0, nz - 1)], ns.at[kind])
    done(r4.at[:, pl.ds(0, nz - 1)], p3s.at[0])
    if early:
        done(rz.at[:, pl.ds(0, nz - 1)], zs.at[0])
        done(rw, ws.at[0])
        done(lim_z.at[pl.ds(0, nz - 1)], vs.at[0])
        done(lim_w, vs.at[1])
    for i in range(5):
        done(lim_c, ms.at[i])


def body(groups, members, partials):
    shots, depth, lateral, width = partials.shape
    nd, nz, rows, cw = depth // groups, members // 2, lateral // members, width // 4
    parts = 4 if rows % 64 == 0 else 1
    rr, edge = rows // parts, min(8, rows)
    early = 2 if parts > 1 else 1
    total = 2 * nd * parts
    steps = total - early
    src = partials.reshape(2, 2, nd, nz, 2, rows, width)
    kind = partials.dtype
    dma = pltpu.SemaphoreType.DMA
    return pl.pallas_call(
        functools.partial(kernel, groups, members),
        out_shape=jax.ShapeDtypeStruct((nd, rows, width), F32),
        in_specs=[pl.BlockSpec(memory_space=pl.ANY)],
        out_specs=pl.BlockSpec(memory_space=pltpu.VMEM),
        scratch_shapes=[
            pltpu.VMEM((2, 2, nd, nz, 2, rows, width), kind),
            pltpu.VMEM((total, 2, nz, 2, rr, 2 * cw), kind),
            pltpu.VMEM((steps, nz, 2, rr, cw), kind),
            pltpu.VMEM((steps, 2, nz, rr, cw), kind),
            pltpu.VMEM((steps, nz, 2, rr, cw), kind),
            pltpu.VMEM((steps, 2, nz, rr, cw), kind),
            pltpu.VMEM((2, steps, nz, rr, cw), kind),
            pltpu.VMEM((2, steps, nz, rr, cw), kind),
            pltpu.VMEM((steps, nz, rr, 2 * cw), F32),
            pltpu.VMEM((steps, nz, rr, 2 * cw), kind),
            pltpu.VMEM((steps, nz, rr, 2 * cw), kind),
            pltpu.VMEM((early, nz, 2, 2, rr, 2 * cw), kind),
            pltpu.VMEM((early, nz, 2, 2, rr, 2 * cw), kind),
            pltpu.VMEM((early, 2, 2, rr, 2 * cw), F32),
            pltpu.VMEM((early, 2, 2, rr, 2 * cw), kind),
            pltpu.VMEM((early, 3, rr, 2 * cw), kind),
            pltpu.VMEM((7, rr, cw), F32),
            pltpu.VMEM((rr, cw), F32),
            pltpu.VMEM((2, rr, cw), F32),
            pltpu.VMEM((2, rr, cw), F32),
            pltpu.VMEM((2, nz, rr, cw), F32),
            pltpu.VMEM((nz, rr, cw), F32),
            pltpu.VMEM((3, rr, cw), F32),
            pltpu.VMEM((nd, rows, width), F32),
            pltpu.VMEM((rows, width), F32),
            pltpu.VMEM((rows, width), F32),
            pltpu.VMEM((nd, edge, width), F32),
            pltpu.VMEM((nd, edge, width), F32),
            dma((2 * nd,)),
            dma((1,)), dma((total,)),
            dma((2,)), dma((2, steps)),
            dma((2,)), dma((2, steps)),
            dma((1,)), dma((steps,)),
            dma((1,)), dma((early,)),
            dma((1,)), dma((early,)),
            dma((5,)), dma((5,)),
            dma((2,)), dma((2,)),
            dma((2,)), dma((2,)),
            dma((4,)), dma((4,)),
            pltpu.SemaphoreType.REGULAR((2,)),
        ],
        compiler_params=pltpu.CompilerParams(collective_id=0, has_side_effects=True, vmem_limit_bytes=51 * 2**20),
    )(src)


def solution(mesh):
    groups, members = mesh.shape["shot"], mesh.shape["tile"]
    return jax.shard_map(
        functools.partial(body, groups, members),
        mesh=mesh,
        in_specs=(P(("shot", "tile"), None, None, None),),
        out_specs=P("shot", "tile", None),
        check_vma=False,
    )
```
